1024 devices in a mesh: expert: 16 (over z_lo), dp: 64 (over x, y, z_hi, core).
Axes of the slice: x: 4, y: 4, z: 32 (z_hi: 2, z_lo: 16; z = z_hi * 16 + z_lo), core: 2. Of those that a mesh axis runs over, the one named last changes fastest.
Arguments:
- gradient: float32 [16, 64, 512, 1024], P('expert', 'dp'), may hold values from -200 to 200
- first_moment: float32 [16, 512, 1024], P('expert', 'dp'), may hold values from -0.6 to 0.6
- second_moment: float32 [16, 512, 1024], P('expert', 'dp'), may hold values from 0.002 to 0.02
- left_basis: float32 [16, 512, 512], P('expert'), may hold values from -1 to 1
- right_basis: float32 [16, 2, 512, 512], P('expert'), may hold values from -1 to 1
Outputs:
- update: float32 [16, 512, 1024], P('expert')
- new_first: float32 [16, 512, 1024], P('expert', 'dp')
- new_second: float32 [16, 512, 1024], P('expert', 'dp')
The draws below stay inside these ranges and needn't reach their ends.
All inputs are finite; a program needn't handle non-finite values.
Results may differ from the reference program's by a relative error of at most 0.000092.
Values sent between devices are 32-bit elements; how exact they have to be, the bound alone decides.
No kernel may reach another device: no remote copies, remote signals or barrier semaphores. Data moves between devices by JAX's collectives and lax.ppermute only.
A program may use at most 32 MiB of HBM per device.

```python
import math
import jax
import jax.numpy as jnp
from jax import lax

BLOCK = 512
RIGHT_BLOCKS = 2
COLS = 1024
EXPERTS = 16
REPLICAS = 64


def orthogonal(key, count):
    raw = jax.random.normal(key, (count, BLOCK, BLOCK), jnp.float32)
    basis, upper = jnp.linalg.qr(raw)
    return basis


def draw_gradient(key, part):
    noise_key, row_key, col_key = jax.random.split(jax.random.fold_in(key, 11), 3)
    row_scale = jnp.exp(jax.random.uniform(row_key, (EXPERTS, 1, BLOCK, 1), jnp.float32, jnp.log(0.5), jnp.log(5.0)))
    col_scale = jnp.exp(jax.random.uniform(col_key, (EXPERTS, 1, 1, COLS), jnp.float32, jnp.log(0.5), jnp.log(5.0)))
    noise = jnp.clip(jax.random.normal(noise_key, (EXPERTS, REPLICAS, BLOCK, COLS), jnp.float32), -6.0, 6.0)
    return noise * row_scale * col_scale


def draw_first_moment(key, part):
    noise_key, row_key = jax.random.split(jax.random.fold_in(key, 23), 2)
    rows = jnp.arange(BLOCK, dtype=jnp.float32) / (BLOCK - 1)
    experts = jnp.arange(EXPERTS, dtype=jnp.float32) / max(EXPERTS - 1, 1)
    ramp = jnp.exp(jnp.log(3.0) * (rows[None, :, None] + experts[:, None, None]) * 0.5)
    noise = jnp.clip(jax.random.normal(noise_key, (EXPERTS, BLOCK, COLS), jnp.float32), -3.0, 3.0)
    jitter = jax.random.uniform(row_key, (EXPERTS, BLOCK, 1), jnp.float32, 0.7, 1.3)
    return 0.05 * noise * ramp * jitter


def draw_left_basis(key, part):
    return orthogonal(jax.random.fold_in(key, 37), EXPERTS)


def draw_right_basis(key, part):
    basis = orthogonal(jax.random.fold_in(key, 41), EXPERTS * RIGHT_BLOCKS)
    return basis.reshape(EXPERTS, RIGHT_BLOCKS, BLOCK, BLOCK)


def level_of(own_key, dims, cuts, smallest, high):
    loudness, own = 1.0, jax.random.fold_in(own_key, 6)
    for position, blocks in cuts:
        steps = jnp.exp(jax.random.uniform(jax.random.fold_in(own, position), (blocks,), jnp.float32, smallest / len(cuts), high / len(cuts)))
        loudness = loudness * jnp.repeat(steps, dims[position] // blocks).reshape([-1 if axis == position else 1 for axis in range(len(dims))])
    return loudness


def setup_inputs(seed: int = 0) -> dict:
    keys = jax.random.split(jax.random.key(seed), 6)
    return {
        "gradient": draw_gradient(jax.random.fold_in(keys[5], 71), 0),
        "first_moment": draw_first_moment(jax.random.fold_in(keys[5], 71), 0),
        "second_moment": jnp.clip(jnp.exp(math.log(0.02) - 2.30258502 * jax.random.uniform(keys[2], (EXPERTS, BLOCK, COLS), jnp.float32) ** level_of(keys[2], (EXPERTS, BLOCK, COLS), ((0, 16), (1, 64)), -0.2, 0.2)), 0.002, 0.02),
        "left_basis": draw_left_basis(jax.random.fold_in(keys[5], 71), 0),
        "right_basis": draw_right_basis(jax.random.fold_in(keys[5], 71), 0),
    }


highest = lax.Precision.HIGHEST

def right_turn(x, basis):
    parts = x.reshape(x.shape[0], x.shape[1], RIGHT_BLOCKS, BLOCK)
    out = jnp.einsum('erbc,ebcd->erbd', parts, basis, precision=highest)
    return out.reshape(x.shape)

def right_back(x, basis):
    parts = x.reshape(x.shape[0], x.shape[1], RIGHT_BLOCKS, BLOCK)
    out = jnp.einsum('erbd,ebcd->erbc', parts, basis, precision=highest)
    return out.reshape(x.shape)

def reference(gradient, first_moment, second_moment, left_basis, right_basis):
    summed = lax.optimization_barrier(jnp.sum(gradient, axis=1))
    left = jnp.einsum('ekr,ekc->erc', left_basis, summed, precision=highest)
    mean = right_turn(left, right_basis) / REPLICAS
    new_first = 0.9 * first_moment + 0.1 * mean
    new_second = 0.95 * second_moment + 0.05 * mean * mean
    normal = new_first / (jnp.sqrt(new_second) + 1e-08)
    scale = jnp.sqrt(jnp.sum(normal * normal) / (EXPERTS * BLOCK * COLS) + 1e-06)
    turned = right_back(normal, right_basis)
    back = jnp.einsum('ekr,erc->ekc', left_basis, turned, precision=highest)
    return (back / scale, new_first, new_second)
```

```python
import jax
import jax.numpy as jnp
from jax import lax
from jax.sharding import Mesh
from jax.sharding import PartitionSpec as P


DP = ("dp_0", "dp_1", "dp_2", "dp_3")
PLANE = ("dp_0", "dp_1")
PLANE_CORE = ("dp_0", "dp_1", "dp_3")
RING = ("expert", "dp_2")
SWAP = [(0, 1), (1, 0)]

highest = lax.Precision.HIGHEST


def rows_dot(a, b):
    return lax.dot_general(a, b, (((0,), (0,)), ((), ())), precision=highest)


def right_turn(values, basis):
    blocks, order = basis.shape[0], basis.shape[1]
    parts = values.reshape(values.shape[0], blocks, order)
    out = jnp.einsum("rbc,bcd->rbd", parts, basis, precision=highest)
    return out.reshape(values.shape)


def right_back(values, basis):
    blocks, order = basis.shape[0], basis.shape[1]
    parts = values.reshape(values.shape[0], blocks, order)
    out = jnp.einsum("rbd,bcd->rbc", parts, basis, precision=highest)
    return out.reshape(values.shape)


def shared_total(tile, axes):
    tiles = jnp.broadcast_to(tile, (lax.axis_size(axes), *tile.shape))
    return jnp.sum(lax.all_to_all(tiles, axes, 0, 0), axis=0)


def along_z(tile, steps):
    ring, experts = lax.axis_size(RING), lax.axis_size("expert")
    place = [z % experts * (ring // experts) + z // experts for z in range(ring)]
    moved = [
        lax.ppermute(tile, RING, [(place[z], place[(z + step) % ring]) for z in range(ring)])
        for step in steps
    ]
    return sum(moved, tile)


def halves(own, other, index):
    return jnp.concatenate(
        (jnp.where(index == 0, own, other), jnp.where(index == 0, other, own)), axis=0
    )


def per_device(gradient, first_moment, second_moment, left_basis, right_basis):
    left, right = left_basis[0], right_basis[0]
    local = gradient[0, 0]
    order, width = local.shape
    replicas = lax.axis_size(DP)
    chips = lax.axis_size(PLANE)
    rows = first_moment.shape[1]
    half = lax.axis_index("dp_2")
    core = lax.axis_index("dp_3")

    columns = jnp.transpose(left).reshape(-1, 2, rows, order)
    here = lax.dynamic_index_in_dim(columns, core, 1, keepdims=False).reshape(-1, order)
    there = lax.dynamic_index_in_dim(columns, 1 - core, 1, keepdims=False).reshape(-1, order)
    sent = jnp.dot(there, local, precision=highest)
    kept = lax.optimization_barrier(jnp.dot(here, local, precision=highest))
    pair = kept + lax.ppermute(sent, "dp_3", SWAP)
    pieces = lax.all_to_all(pair.reshape(chips, 2 * rows, width), PLANE, 0, 0)
    partial = jnp.sum(pieces, axis=0)

    moments = jnp.concatenate((first_moment[0], second_moment[0]), axis=0)
    moments_there = lax.ppermute(moments, "dp_2", SWAP)
    first = halves(first_moment[0], moments_there[:rows], half)
    second = halves(second_moment[0], moments_there[rows:], half)

    summed = partial + lax.ppermute(partial, "dp_2", SWAP)
    mean = right_turn(summed, right) / replicas
    new_first = 0.9 * first + 0.1 * mean
    new_second = 0.95 * second + 0.05 * mean * mean
    normal = new_first / (jnp.sqrt(new_second) + 1e-08)

    squares = jnp.broadcast_to(jnp.sum(normal * normal), (8, 128))
    expert_total = shared_total(squares, PLANE_CORE)
    turned, expert_total = lax.optimization_barrier((right_back(normal, right), expert_total))
    total = along_z(along_z(expert_total, (1, -1, 2)), (4, -4, 8))[0, 0]
    count = lax.axis_size("expert") * order * width
    scale = jnp.sqrt(total / count + 1e-06)
    ours = lax.all_to_all(jnp.broadcast_to(turned, (chips, 2 * rows, width)), PLANE, 0, 0)
    ours = ours.reshape(-1, width)
    theirs = lax.ppermute(ours, "dp_3", SWAP)
    back = rows_dot(here, ours) + rows_dot(there, theirs)
    own = lambda x: lax.dynamic_slice_in_dim(x, half * rows, rows, 0)
    return ((back / scale)[None], own(new_first)[None], own(new_second)[None])


def solution(mesh):
    split = Mesh(
        mesh.devices.reshape(mesh.shape["expert"], 4, 4, 2, 2),
        ("expert", "dp_0", "dp_1", "dp_2", "dp_3"),
    )
    in_specs = (
        P("expert", DP, None, None),
        P("expert", DP, None),
        P("expert", DP, None),
        P("expert", None, None),
        P("expert", None, None, None),
    )
    out_specs = (P("expert", None, None), P("expert", DP, None), P("expert", DP, None))
    return jax.shard_map(
        per_device, mesh=split, in_specs=in_specs, out_specs=out_specs, check_vma=False
    )
```

```python
import jax
import jax.numpy as jnp
from jax import lax
from jax.sharding import Mesh
from jax.sharding import PartitionSpec as P


DP = ("dp_0", "dp_1", "dp_2", "dp_3")
PLANE = ("dp_0", "dp_1")
PLANE_CORE = ("dp_0", "dp_1", "dp_3")
RING = ("expert", "dp_2")
SWAP = [(0, 1), (1, 0)]

highest = lax.Precision.HIGHEST
high = lax.Precision.HIGH


def rows_dot(a, b):
    return lax.dot_general(a, b, (((0,), (0,)), ((), ())), precision=high)


def right_turn(values, basis):
    blocks, order = basis.shape[0], basis.shape[1]
    parts = values.reshape(values.shape[0], blocks, order)
    out = jnp.einsum("rbc,bcd->rbd", parts, basis, precision=high)
    return out.reshape(values.shape)


def right_back(values, basis):
    blocks, order = basis.shape[0], basis.shape[1]
    parts = values.reshape(values.shape[0], blocks, order)
    out = jnp.einsum("rbd,bcd->rbc", parts, basis, precision=high)
    return out.reshape(values.shape)


def shared_total(tile, axes):
    tiles = jnp.broadcast_to(tile, (lax.axis_size(axes), *tile.shape))
    return jnp.sum(lax.all_to_all(tiles, axes, 0, 0), axis=0)


def along_z(tile, steps):
    ring, experts = lax.axis_size(RING), lax.axis_size("expert")
    place = [z % experts * (ring // experts) + z // experts for z in range(ring)]
    moved = [
        lax.ppermute(tile, RING, [(place[z], place[(z + step) % ring]) for z in range(ring)])
        for step in steps
    ]
    return sum(moved, tile)


def halves(own, other, index):
    return jnp.concatenate(
        (jnp.where(index == 0, own, other), jnp.where(index == 0, other, own)), axis=0
    )


def per_device(gradient, first_moment, second_moment, left_basis, right_basis):
    left, right = left_basis[0], right_basis[0]
    local = gradient[0, 0]
    order, width = local.shape
    replicas = lax.axis_size(DP)
    chips = lax.axis_size(PLANE)
    rows = first_moment.shape[1]
    half = lax.axis_index("dp_2")
    core = lax.axis_index("dp_3")

    columns = jnp.transpose(left).reshape(-1, 2, rows, order)
    here = lax.dynamic_index_in_dim(columns, core, 1, keepdims=False).reshape(-1, order)
    there = lax.dynamic_index_in_dim(columns, 1 - core, 1, keepdims=False).reshape(-1, order)
    sent = jnp.dot(there, local, precision=highest)
    kept = lax.optimization_barrier(jnp.dot(here, local, precision=highest))
    pair = kept + lax.ppermute(sent, "dp_3", SWAP)
    pieces = lax.all_to_all(pair.reshape(chips, 2 * rows, width), PLANE, 0, 0)
    partial = jnp.sum(pieces, axis=0)

    moments = jnp.concatenate((first_moment[0], second_moment[0]), axis=0)
    moments_there = lax.ppermute(moments, "dp_2", SWAP)
    first = halves(first_moment[0], moments_there[:rows], half)
    second = halves(second_moment[0], moments_there[rows:], half)

    summed = partial + lax.ppermute(partial, "dp_2", SWAP)
    mean = right_turn(summed, right) / replicas
    new_first = 0.9 * first + 0.1 * mean
    new_second = 0.95 * second + 0.05 * mean * mean
    normal = new_first / (jnp.sqrt(new_second) + 1e-08)

    squares = jnp.broadcast_to(jnp.sum(normal * normal), (8, 128))
    near = along_z(squares, (1, -1, 2))
    turned = right_back(normal, right)
    ours = lax.all_to_all(jnp.broadcast_to(turned, (chips, 2 * rows, width)), PLANE, 0, 0)
    ours = ours.reshape(-1, width)
    theirs = lax.ppermute(ours, "dp_3", SWAP)
    far = along_z(near, (4, -4, 8))
    total = shared_total(far, PLANE_CORE)[0, 0]
    count = lax.axis_size("expert") * order * width
    scale = jnp.sqrt(total / count + 1e-06)
    back = lax.optimization_barrier(rows_dot(here, ours) + rows_dot(there, theirs))
    own = lambda x: lax.dynamic_slice_in_dim(x, half * rows, rows, 0)
    return ((back * (1.0 / scale))[None], own(new_first)[None], own(new_second)[None])


def solution(mesh):
    split = Mesh(
        mesh.devices.reshape(mesh.shape["expert"], 4, 4, 2, 2),
        ("expert", "dp_0", "dp_1", "dp_2", "dp_3"),
    )
    in_specs = (
        P("expert", DP, None, None),
        P("expert", DP, None),
        P("expert", DP, None),
        P("expert", None, None),
        P("expert", None, None, None),
    )
    out_specs = (P("expert", None, None), P("expert", DP, None), P("expert", DP, None))
    return jax.shard_map(
        per_device, mesh=split, in_specs=in_specs, out_specs=out_specs, check_vma=False
    )
```

```python
import jax
import jax.numpy as jnp
from jax import lax
from jax.sharding import Mesh
from jax.sharding import PartitionSpec as P


DP = ("dp_0", "dp_1", "dp_2", "dp_3")
PLANE = ("dp_0", "dp_1")
PLANE_CORE = ("dp_0", "dp_1", "dp_3")
CHIPS = ("expert", "dp_0", "dp_1", "dp_2")
SWAP = [(0, 1), (1, 0)]

highest = lax.Precision.HIGHEST
high = lax.Precision.HIGH


def rows_dot(a, b):
    return lax.dot_general(a, b, (((0,), (0,)), ((), ())), precision=high)


def right_turn(values, basis):
    blocks, order = basis.shape[0], basis.shape[1]
    parts = values.reshape(values.shape[0], blocks, order)
    out = jnp.einsum("rbc,bcd->rbd", parts, basis, precision=high)
    return out.reshape(values.shape)


def right_back(values, basis):
    blocks, order = basis.shape[0], basis.shape[1]
    parts = values.reshape(values.shape[0], blocks, order)
    out = jnp.einsum("rbd,bcd->rbc", parts, basis, precision=high)
    return out.reshape(values.shape)


def shared_total(tile, axes):
    tiles = jnp.broadcast_to(tile, (lax.axis_size(axes), *tile.shape))
    return jnp.sum(lax.all_to_all(tiles, axes, 0, 0), axis=0)


def along_z(tile):
    experts, split_x, split_y, split_z = (lax.axis_size(axis) for axis in CHIPS)
    ring = experts * split_z

    def index(place, p):
        e, z = place % experts, place // experts
        return (e * split_x * split_y + p) * split_z + z

    pairs = [
        (index(place, p), index((place + p - experts // 2) % ring, p))
        for place in range(ring)
        for p in range(split_x * split_y)
    ]
    return lax.ppermute(tile, CHIPS, pairs)


def halves(own, other, index):
    return jnp.concatenate(
        (jnp.where(index == 0, own, other), jnp.where(index == 0, other, own)), axis=0
    )


def per_device(gradient, first_moment, second_moment, left_basis, right_basis):
    left, right = left_basis[0], right_basis[0]
    local = gradient[0, 0]
    order, width = local.shape
    replicas = lax.axis_size(DP)
    chips = lax.axis_size(PLANE)
    rows = first_moment.shape[1]
    half = lax.axis_index("dp_2")
    core = lax.axis_index("dp_3")

    columns = jnp.transpose(left).reshape(-1, 2, rows, order)
    here = lax.dynamic_index_in_dim(columns, core, 1, keepdims=False).reshape(-1, order)
    there = lax.dynamic_index_in_dim(columns, 1 - core, 1, keepdims=False).reshape(-1, order)
    sent = jnp.dot(there, local, precision=highest)
    kept = lax.optimization_barrier(jnp.dot(here, local, precision=highest))
    pair = kept + lax.ppermute(sent, "dp_3", SWAP)
    pieces = lax.all_to_all(pair.reshape(chips, 2 * rows, width), PLANE, 0, 0)
    partial = jnp.sum(pieces, axis=0)

    moments = jnp.concatenate((first_moment[0], second_moment[0]), axis=0)
    moments_there = lax.ppermute(moments, "dp_2", SWAP)
    first = halves(first_moment[0], moments_there[:rows], half)
    second = halves(second_moment[0], moments_there[rows:], half)

    summed = partial + lax.ppermute(partial, "dp_2", SWAP)
    mean = right_turn(summed, right) / replicas
    new_first = 0.9 * first + 0.1 * mean
    new_second = 0.95 * second + 0.05 * mean * mean
    normal = new_first / (jnp.sqrt(new_second) + 1e-08)

    squares = jnp.broadcast_to(jnp.sum(normal * normal), (8, 128))
    expert_sum = shared_total(squares, PLANE_CORE)
    turned = right_back(normal, right)
    ours = lax.all_to_all(jnp.broadcast_to(turned, (chips, 2 * rows, width)), PLANE, 0, 0)
    ours = ours.reshape(-1, width)
    theirs = lax.ppermute(ours, "dp_3", SWAP)
    another = along_z(expert_sum)
    total = shared_total(another, PLANE)[0, 0]
    count = lax.axis_size("expert") * order * width
    scale = jnp.sqrt(total / count + 1e-06)
    back = rows_dot(here, ours)
    back = back + rows_dot(there, theirs)
    own = lambda x: lax.dynamic_slice_in_dim(x, half * rows, rows, 0)
    return ((back * (1.0 / scale))[None], own(new_first)[None], own(new_second)[None])


def solution(mesh):
    split = Mesh(
        mesh.devices.reshape(mesh.shape["expert"], 4, 4, 2, 2),
        ("expert", "dp_0", "dp_1", "dp_2", "dp_3"),
    )
    in_specs = (
        P("expert", DP, None, None),
        P("expert", DP, None),
        P("expert", DP, None),
        P("expert", None, None),
        P("expert", None, None, None),
    )
    out_specs = (P("expert", None, None), P("expert", DP, None), P("expert", DP, None))
    return jax.shard_map(
        per_device, mesh=split, in_specs=in_specs, out_specs=out_specs, check_vma=False
    )
```

```python
import jax
import jax.numpy as jnp
from jax import lax
from jax.sharding import Mesh
from jax.sharding import PartitionSpec as P


DP = ("dp_0", "dp_1", "dp_2", "dp_3")
PLANE = ("dp_0", "dp_1")
PLANE_CORE = ("dp_0", "dp_1", "dp_3")
CHIPS = ("expert", "dp_0", "dp_1", "dp_2")
SWAP = [(0, 1), (1, 0)]

highest = lax.Precision.HIGHEST
high = lax.Precision.HIGH


def rows_dot(a, b):
    return lax.dot_general(a, b, (((0,), (0,)), ((), ())), precision=high)


def right_turn(values, basis):
    blocks, order = basis.shape[0], basis.shape[1]
    parts = values.reshape(values.shape[0], blocks, order)
    out = jnp.einsum("rbc,bcd->rbd", parts, basis, precision=high)
    return out.reshape(values.shape)


def turned_blocks(values, left, basis):
    blocks = basis.shape[0]
    parts = jnp.split(values, blocks, axis=1)
    return [
        rows_dot(left, lax.dot_general(part, basis[b], (((1,), (1,)), ((), ())), precision=high))
        for b, part in enumerate(parts)
    ]


def shared_total(tile, axes):
    tiles = jnp.broadcast_to(tile, (lax.axis_size(axes), *tile.shape))
    return jnp.sum(lax.all_to_all(tiles, axes, 0, 0), axis=0)


def along_z(tile):
    experts, split_x, split_y, split_z = (lax.axis_size(axis) for axis in CHIPS)
    ring = experts * split_z

    def index(place, p):
        e, z = place % experts, place // experts
        return (e * split_x * split_y + p) * split_z + z

    pairs = [
        (index(place, p), index((place + p - experts // 2) % ring, p))
        for place in range(ring)
        for p in range(split_x * split_y)
    ]
    return lax.ppermute(tile, CHIPS, pairs)


def halves(own, other, index):
    return jnp.concatenate(
        (jnp.where(index == 0, own, other), jnp.where(index == 0, other, own)), axis=0
    )


def per_device(gradient, first_moment, second_moment, left_basis, right_basis):
    left, right = left_basis[0], right_basis[0]
    local = gradient[0, 0]
    order, width = local.shape
    replicas = lax.axis_size(DP)
    chips = lax.axis_size(PLANE)
    rows = first_moment.shape[1]
    half = lax.axis_index("dp_2")
    core = lax.axis_index("dp_3")

    columns = jnp.transpose(left).reshape(-1, 2, rows, order)
    here = lax.dynamic_index_in_dim(columns, core, 1, keepdims=False).reshape(-1, order)
    there = lax.dynamic_index_in_dim(columns, 1 - core, 1, keepdims=False).reshape(-1, order)
    sent = jnp.dot(there, local, precision=highest)
    kept = lax.optimization_barrier(jnp.dot(here, local, precision=highest))
    pair = kept + lax.ppermute(sent, "dp_3", SWAP)
    pieces = lax.all_to_all(pair.reshape(chips, 2 * rows, width), PLANE, 0, 0)
    partial = jnp.sum(pieces, axis=0)

    moments = jnp.concatenate((first_moment[0], second_moment[0]), axis=0)
    moments_there = lax.ppermute(moments, "dp_2", SWAP)
    first = halves(first_moment[0], moments_there[:rows], half)
    second = halves(second_moment[0], moments_there[rows:], half)

    summed = partial + lax.ppermute(partial, "dp_2", SWAP)
    mean = right_turn(summed, right) / replicas
    new_first = 0.9 * first + 0.1 * mean
    new_second = 0.95 * second + 0.05 * mean * mean
    normal = new_first / (jnp.sqrt(new_second) + 1e-08)

    ours = lax.all_to_all(jnp.broadcast_to(normal, (chips, 2 * rows, width)), PLANE, 0, 0)
    ours = ours.reshape(-1, width)
    theirs = lax.ppermute(ours, "dp_3", SWAP)
    squares = jnp.broadcast_to(jnp.sum(ours * ours), (8, 128))
    another = along_z(squares)
    total = shared_total(another, PLANE_CORE)[0, 0]
    count = lax.axis_size("expert") * order * width
    scale = jnp.sqrt(total / count + 1e-06)
    back = turned_blocks(ours, here, right)
    more = turned_blocks(theirs, there, right)
    back = lax.optimization_barrier([a + b for a, b in zip(back, more)])
    back = jnp.concatenate([block * (1.0 / scale) for block in back], axis=1)
    own = lambda x: lax.dynamic_slice_in_dim(x, half * rows, rows, 0)
    return (back[None], own(new_first)[None], own(new_second)[None])


def solution(mesh):
    split = Mesh(
        mesh.devices.reshape(mesh.shape["expert"], 4, 4, 2, 2),
        ("expert", "dp_0", "dp_1", "dp_2", "dp_3"),
    )
    in_specs = (
        P("expert", DP, None, None),
        P("expert", DP, None),
        P("expert", DP, None),
        P("expert", None, None),
        P("expert", None, None, None),
    )
    out_specs = (P("expert", None, None), P("expert", DP, None), P("expert", DP, None))
    return jax.shard_map(
        per_device, mesh=split, in_specs=in_specs, out_specs=out_specs, check_vma=False
    )
```
